32 devices in a mesh: tgt: 8 (over y, x, core), src: 4 (over z).
Axes of the slice: x: 2, y: 2, z: 4, core: 2. Of those that a mesh axis runs over, the one named last changes fastest.
Arguments:
- fibre_points: float32 [3, 64, 64], P(None, ('tgt', 'src')), may hold values from -6 to 6
- shell_points: float32 [3, 128, 64], P(None, 'tgt', 'src'), may hold values from -7 to 7, as said below
- bending: float32 [64, 64], replicated, may hold values from -0.12 to 0.12
- shell_inverse: bfloat16 [3, 128, 64, 3, 64, 128], P(None, 'tgt', None, None, 'src'), may hold values from -0.0390625 to 0.0390625
Outputs:
- fibre_velocity: float32 [3, 64, 64], P(None, ('tgt', 'src'))
- shell_density: float32 [3, 128, 64], P(None, 'tgt', 'src')
The draws below stay inside these ranges and needn't reach their ends.
Inputs may be any that keep to these rules, and one draw needn't show every extreme that they name: `shell_points`: every shell node lies on the sphere of radius 7 about the anchor.
All inputs are finite; a program needn't handle non-finite values.
Results may differ from the reference program's by a relative error of at most 0.0029.
Values may be sent and summed in bfloat16 or wider, within the bound.
A program may use at most 64 MiB of HBM per device.

```python
import math
import jax
import jax.numpy as jnp
from jax import lax

NODES = 64
NSA = 128
NSB = 64
ITERS = 1
FIBRES = 64
SHELL = 8192


def draw_shell_points(key, part):
    height_key, angle_key = jax.random.split(key)
    height = jax.random.uniform(height_key, (NSA, NSB), jnp.float32, -1.0, 1.0)
    angle = jax.random.uniform(angle_key, (NSA, NSB), jnp.float32, -math.pi, math.pi)
    radial = jnp.sqrt(jnp.maximum(1.0 - height * height, 0.0))
    return 7.0 * jnp.stack([radial * jnp.cos(angle), radial * jnp.sin(angle), height])


def steps_of(own_key, extent, cuts, smallest, top_value):
    def one(dim, parts):
        steps = jax.random.uniform(jax.random.fold_in(jax.random.fold_in(own_key, 6), dim), (parts,), jnp.float32, smallest / len(cuts), top_value / len(cuts))
        return jnp.repeat(jnp.exp(steps), extent[dim] // parts).reshape((-1,) + (1,) * (len(extent) - dim - 1))

    loudness = one(*cuts[0])
    for cut in cuts[1:]:
        loudness = loudness * one(*cut)
    return loudness


def bell_draw(key, extent, spread, bound, cuts=(), dtype=jnp.bfloat16):
    factor_of = steps_of(key, extent, cuts, -0.22, 0.18) if cuts else 1.0
    drawn = jax.random.normal(key, extent, jnp.float32) * spread * factor_of
    return jnp.minimum(jnp.maximum(drawn, -bound), bound).astype(dtype)


def setup_inputs(seed: int = 0) -> dict:
    keys = jax.random.split(jax.random.key(seed), 5)
    return {
        "fibre_points": bell_draw(keys[0], (3, FIBRES, NODES), 1.0, 6.0, ((1, 32),), jnp.float32),
        "shell_points": draw_shell_points(jax.random.fold_in(keys[4], 71), 0),
        "bending": bell_draw(keys[2], (NODES, NODES), 0.02, 0.12, (), jnp.float32),
        "shell_inverse": bell_draw(keys[3], (3, NSA, NSB, 3, NSB, NSA), (3 * SHELL) ** -0.5, 0.0390625, ((1, 8), (4, 4))),
    }


mobility = 1.0 / (8.0 * math.pi)
soften_sq = 0.0025
time_step = 0.5

def stokes_flow(targets, sources, strength):
    delta_x = targets[0][:, None] - sources[0][None, :]
    delta_y = targets[1][:, None] - sources[1][None, :]
    delta_z = targets[2][:, None] - sources[2][None, :]
    dist_sq = delta_x * delta_x + delta_y * delta_y + delta_z * delta_z
    inv_root = lax.rsqrt(dist_sq + soften_sq)
    inv_cubed = inv_root * inv_root * inv_root
    projection = (delta_x * strength[0][None, :] + delta_y * strength[1][None, :] + delta_z * strength[2][None, :]) * inv_cubed
    diagonal_part = (dist_sq + 2.0 * soften_sq) * inv_cubed
    flow_x = lax.optimization_barrier(jnp.sum(diagonal_part * strength[0][None, :] + projection * delta_x, axis=1))
    flow_y = lax.optimization_barrier(jnp.sum(diagonal_part * strength[1][None, :] + projection * delta_y, axis=1))
    flow_z = lax.optimization_barrier(jnp.sum(diagonal_part * strength[2][None, :] + projection * delta_z, axis=1))
    return mobility * jnp.stack([flow_x, flow_y, flow_z])

def blocked_flow(targets, sources, strength):
    column_count = targets.shape[1]
    block_size = math.gcd(column_count, 128)
    blocks = targets.reshape(3, column_count // block_size, block_size).transpose(1, 0, 2)

    def one_block(target_block):
        return stokes_flow(target_block, sources, strength)
    result = lax.map(one_block, blocks)
    return result.transpose(1, 0, 2).reshape(3, column_count)

def reference(fibre_points, shell_points, bending, shell_inverse):
    points = fibre_points
    shell_flat = shell_points.reshape(3, -1)
    matrix = shell_inverse.reshape(3 * SHELL, 3 * SHELL)
    fibre_count = FIBRES * NODES
    velocity = jnp.zeros(points.shape, jnp.float32)
    density = jnp.zeros(shell_points.shape, jnp.float32)
    for iteration in range(ITERS):
        forces = -jnp.einsum('cfm,nm->cfn', points, bending, precision=lax.Precision.HIGHEST)
        sources = points.reshape(3, -1)
        targets = jnp.concatenate([sources, shell_flat], axis=1)
        flow_all = blocked_flow(targets, sources, forces.reshape(3, -1))
        fibre_flow = flow_all[:, :fibre_count].reshape(points.shape)
        shell_flow = flow_all[:, fibre_count:].reshape(3, NSA, NSB)
        columns = shell_flow.astype(jnp.bfloat16).transpose(0, 2, 1).reshape(-1)
        density = -jnp.dot(matrix, columns, preferred_element_type=jnp.float32).reshape(3, NSA, NSB)
        shell_back = blocked_flow(sources, shell_flat, density.reshape(3, -1)).reshape(points.shape)
        velocity = fibre_flow + shell_back
        if iteration + 1 < ITERS:
            points = points + time_step * velocity
    return (velocity, density)
```

```python
import functools
import math

import jax
import jax.numpy as jnp
from jax import lax
from jax.experimental import pallas as pl
from jax.experimental.pallas import tpu as pltpu
from jax.sharding import PartitionSpec as P

mobility = 1.0 / (8.0 * math.pi)
soften_sq = 0.0025
LANES = 128
SUB = 8
HIGHEST = lax.Precision.HIGHEST
MESH = pl.DeviceIdType.MESH
f32 = jnp.float32


def iotas(rows=SUB):
    lane = lax.broadcasted_iota(jnp.int32, (rows, LANES), 1)
    sub = lax.broadcasted_iota(jnp.int32, (rows, LANES), 0)
    return lane, sub


def flow(src_ref, start, count, targets, accs, unroll):
    unroll = math.gcd(unroll, count)

    def body(i, accs):
        accs = list(accs)
        for u in range(unroll):
            j = start + i * unroll + u
            sx, sy, sz, gx, gy, gz = [src_ref[j, c] for c in range(6)]
            for g, (tx, ty, tz) in enumerate(targets):
                dx, dy, dz = tx - sx, ty - sy, tz - sz
                q = dx * dx + dy * dy + (dz * dz + soften_sq)
                inv = lax.rsqrt(q)
                cubed = inv * inv * inv
                proj = (dx * gx + dy * gy + dz * gz) * cubed
                diag = (q + soften_sq) * cubed
                accs[3 * g] += diag * gx + proj * dx
                accs[3 * g + 1] += diag * gy + proj * dy
                accs[3 * g + 2] += diag * gz + proj * dz
        return tuple(accs)

    return lax.fori_loop(0, count // unroll, body, tuple(accs))


def fold_rows(rows, sub):
    def step(a, b, width):
        low = (sub & width) == 0
        up = a + pltpu.roll(a, SUB - width, 0)
        down = b + pltpu.roll(b, width, 0)
        return jnp.where(low, up, down)

    width = 4
    level = rows
    half = len(rows) // 2
    while half >= 1:
        level = [step(level[i], level[i + half], width) for i in range(half)]
        width //= 2
        half //= 2
    return level[0]


def kernel(
    nt, ns, fib_ref, shell_ref, bend_ref, mat_ref, vel_ref, den_ref,
    mat, gbuf, pbuf, dbuf, cbuf, part, rbuf, tbs, tbf, wide, src1, src2, fib_acc, weave,
    posblk, denblk, colblk, ptblk, lane_ref,
    mat_sem, g_send, g_recv, p_send, p_recv, c_send, c_recv, r_send, r_recv, d_send, d_recv,
):
    t, s = lax.axis_index("tgt"), lax.axis_index("src")
    n_dev = nt * ns
    al, ql = shell_ref.shape[1], shell_ref.shape[2]
    fl, nodes = fib_ref.shape[1], fib_ref.shape[2]
    fib_groups = LANES // SUB
    qv = min(ql, LANES // al)
    nvec = ql // qv
    lane_ref[...] = iotas(ql)[0]
    sub = iotas()[1]
    sub16 = iotas(ql)[1]
    lane, lane16 = lane_ref[pl.ds(0, SUB), :], lane_ref[...]

    def fetch(k):
        to = lax.rem(s + 1 + k, ns)
        return pltpu.make_async_copy(
            mat_ref.at[:, :, pl.ds(to * ql, ql)], mat.at[k], mat_sem.at[k]
        )

    for k in range(ns):
        fetch(k).start()

    def peer(i):
        return {"tgt": lax.rem(t + lax.rem(i, nt), nt), "src": lax.rem(s + i // nt, ns)}

    gbuf[...] = jnp.zeros_like(gbuf)
    barrier = pltpu.get_barrier_semaphore()

    def greet(i, _):
        pl.semaphore_signal(barrier, inc=1, device_id=peer(i), device_id_type=MESH)
        return 0

    lax.fori_loop(1, n_dev, greet, 0)

    ptblk[...] = jnp.zeros_like(ptblk)
    posblk[...] = jnp.zeros_like(posblk)
    denblk[...] = jnp.zeros_like(denblk)
    points = jnp.concatenate([fib_ref[:, f, :] for f in range(fl)], axis=1)
    ptblk[pl.ds(0, 3), :] = points
    bend = bend_ref[...]
    blank = jnp.zeros_like(bend)
    weave[...] = jnp.concatenate(
        [
            jnp.concatenate([bend if i == j else blank for j in range(fl)], axis=1)
            for i in range(fl)
        ],
        axis=0,
    )

    def spread(a, reps):
        out = []
        for c in range(3):
            row = shell_ref[c, pl.ds(a, 1), :]
            eye = lax.broadcasted_iota(jnp.int32, (ql, ql), 0) == lax.broadcasted_iota(
                jnp.int32, (ql, ql), 1
            )
            col = jnp.sum(jnp.where(eye, 1.0, 0.0) * row, axis=1, keepdims=True)
            wide_col = jnp.broadcast_to(col, (ql, LANES))
            tbs[a, c] = wide_col
            out.append(jnp.where(lax.rem(lane16, al) == a, wide_col, reps[c]))
        return tuple(out)

    reps = lax.fori_loop(0, al, spread, tuple(jnp.zeros((ql, LANES), f32) for _ in range(3)))

    def weave_rows(block, values):
        for c in range(3):
            for h in range(nvec):
                piece = values[c][h * qv:(h + 1) * qv]
                hit = lax.div(lane16[:qv], al) == sub16[:qv]
                block[pl.ds(c * nvec + h, 1), :] = jnp.sum(
                    jnp.where(hit, piece, 0.0), axis=0, keepdims=True
                )

    weave_rows(posblk, reps)

    def spread_fibre(g, _):
        for c in range(3):
            row = ptblk[pl.ds(c, 1), :]
            hit = jnp.where(lane == sub + g * SUB, 1.0, 0.0)
            col = jnp.sum(hit * row, axis=1, keepdims=True)
            tbf[g, c] = jnp.broadcast_to(col, (SUB, LANES))
        return 0

    lax.fori_loop(0, fib_groups, spread_fibre, 0)

    me = s * nt + t
    gbuf[me] = ptblk[...]
    pbuf[me] = posblk[...]
    pl.semaphore_wait(barrier, n_dev - 1)

    def spread_out(block, buf, rows, send, recv):
        def one(i, _):
            pltpu.make_async_remote_copy(
                src_ref=block.at[pl.ds(0, rows)],
                dst_ref=buf.at[me, pl.ds(0, rows)],
                send_sem=send,
                recv_sem=recv.at[s],
                device_id=peer(i),
                device_id_type=MESH,
            ).start()
            return 0

        lax.fori_loop(1, n_dev, one, 0)

    def arrived(buf, rows, recv, k):
        frm = lax.rem(s + k, ns)
        ref = buf.at[pl.ds(0, nt if k else nt - 1), pl.ds(0, rows)]
        pltpu.make_async_copy(ref, ref, recv.at[frm]).wait()

    def sent(buf, rows, send):
        ref = buf.at[pl.ds(0, n_dev - 1), pl.ds(0, rows)]
        pltpu.make_async_copy(ref, ref, send).wait()

    spread_out(ptblk, gbuf, 3, g_send, g_recv)
    spread_out(posblk, pbuf, SUB, p_send, p_recv)
    for k in range(ns):
        arrived(gbuf, 3, g_recv, k)

    all_points = gbuf[...].reshape(n_dev * SUB, LANES)
    wide[...] = (
        lax.dot_general(
            all_points, weave[...], (((1,), (1,)), ((), ())),
            precision=HIGHEST, preferred_element_type=f32,
        )
        * (-mobility)
    ).reshape(n_dev, SUB, LANES)

    def plane(j, _):
        for c in range(3):
            src1[j, c] = jnp.broadcast_to(gbuf[j, pl.ds(c, 1), :], (SUB, LANES))
            src1[j, c + 3] = jnp.broadcast_to(wide[j, pl.ds(c, 1), :], (SUB, LANES))
        return 0

    lax.fori_loop(0, n_dev, plane, 0)
    halves = ql // SUB
    zero = jnp.zeros((SUB, LANES), f32)

    def shell_targets(a, cols):
        groups = [
            tuple(tbs[a, c, pl.ds(h * SUB, SUB), :] for c in range(3)) for h in range(halves)
        ]
        accs = flow(src1, 0, n_dev, groups, [zero] * (3 * halves), 4)
        here = lane == t * al + a
        return tuple(
            jnp.where(here, jnp.sum(accs[i], axis=1, keepdims=True), cols[i])
            for i in range(3 * halves)
        )

    cols = lax.fori_loop(0, al, shell_targets, tuple([zero] * (3 * halves)))
    for c in range(3):
        colblk[c] = jnp.concatenate(
            [cols[3 * h + c] for h in range(halves)], axis=0
        ).astype(jnp.bfloat16)
    cbuf[t] = colblk[...]

    def send_cols(i, _):
        pltpu.make_async_remote_copy(
            src_ref=colblk, dst_ref=cbuf.at[t], send_sem=c_send, recv_sem=c_recv,
            device_id={"tgt": lax.rem(t + i, nt), "src": s}, device_id_type=MESH,
        ).start()
        return 0

    lax.fori_loop(1, nt, send_cols, 0)

    def fibre_targets(src_ref, start, count, first):
        def one(i, _):
            groups = [tuple(tbf[2 * i + h, c] for c in range(3)) for h in range(2)]
            accs = [
                zero if first else fib_acc[2 * i + h, c] for h in range(2) for c in range(3)
            ]
            accs = flow(src_ref, start, count, groups, accs, 4)
            for h in range(2):
                for c in range(3):
                    fib_acc[2 * i + h, c] = accs[3 * h + c]
            return 0

        lax.fori_loop(0, fib_groups // 2, one, 0)

    fibre_targets(src1, 0, n_dev, True)

    others = cbuf.at[pl.ds(0, nt - 1)]
    pltpu.make_async_copy(others, others, c_recv).wait()
    v = lax.fori_loop(
        0, nt, lambda i, total: total + cbuf[i].astype(f32), jnp.zeros(cbuf.shape[1:], f32)
    )

    def send_part(k):
        to = lax.rem(s + 1 + k, ns)
        return pltpu.make_async_remote_copy(
            src_ref=part.at[k], dst_ref=rbuf.at[k],
            send_sem=r_send.at[k], recv_sem=r_recv.at[k],
            device_id={"tgt": t, "src": to}, device_id_type=MESH,
        )

    def place(a, folded, dens):
        here = lax.rem(lane, al) == a
        return tuple(
            jnp.where(here, jnp.sum(y, axis=1, keepdims=True), d) for y, d in zip(folded, dens)
        )

    for k in range(ns):
        fetch(k).wait()

        def row_block(a, carry):
            folded, dens = carry
            dens = place(a - 1, folded, dens)
            new = []
            for x in range(3):
                for h in range(halves):
                    rows = []
                    for r in range(SUB):
                        prod = mat[k, x, a, h * SUB + r].astype(f32) * v
                        both = prod[0] + prod[1] + prod[2]
                        rows.append(
                            sum(both[i * SUB:(i + 1) * SUB] for i in range(halves))
                        )
                    new.append(fold_rows(rows, sub))
            return tuple(new), dens

        empty = tuple([zero] * (3 * halves))
        folded, dens = lax.fori_loop(0, al, row_block, (empty, empty))
        dens = place(al - 1, folded, dens)
        for x in range(3):
            for h in range(halves):
                part[k, x, pl.ds(h * SUB, SUB), :] = dens[x * halves + h]
        if k < ns - 1:
            send_part(k).start()

    total = part[ns - 1]
    for k in range(ns - 1):
        send_part(k).wait_recv()
        total = total + rbuf[k]
    total = -total
    weave_rows(denblk, [total[x] for x in range(3)])
    dbuf[me] = denblk[...]
    spread_out(denblk, dbuf, SUB, d_send, d_recv)

    pick = max(al, SUB)
    pl_lane, pl_sub = iotas(pick)
    eye = jnp.where(pl_lane == pl_sub, 1.0, 0.0).astype(f32)
    for x in range(3):
        den_ref[x] = lax.dot_general(
            eye, total[x], (((1,), (1,)), ((), ())), precision=HIGHEST, preferred_element_type=f32
        )[:al]

    for k in range(ns):
        arrived(pbuf, SUB, p_recv, k)
        arrived(dbuf, SUB, d_recv, k)
        base = lax.rem(s + k, ns) * nt

        def plane_back(j, _):
            for h in range(nvec):
                for c in range(3):
                    r = pl.ds(c * nvec + h, 1)
                    src2[j * nvec + h, c] = jnp.broadcast_to(pbuf[base + j, r, :], (SUB, LANES))
                    src2[j * nvec + h, c + 3] = jnp.broadcast_to(
                        dbuf[base + j, r, :] * mobility, (SUB, LANES)
                    )
            return 0

        lax.fori_loop(0, nt, plane_back, 0)
        fibre_targets(src2, 0, nt * nvec, False)

    def gather_rows(g, rows):
        hit = lane == sub + g * SUB
        return tuple(
            rows[c] + jnp.where(hit, jnp.sum(fib_acc[g, c], axis=1, keepdims=True), 0.0)
            for c in range(3)
        )

    rows = lax.fori_loop(0, fib_groups, gather_rows, (zero,) * 3)
    for c in range(3):
        row = jnp.sum(rows[c], axis=0, keepdims=True)
        for f in range(fl):
            vel_ref[c, pl.ds(f, 1), :] = row[:, f * nodes:(f + 1) * nodes]

    sent(gbuf, 3, g_send)
    sent(pbuf, SUB, p_send)
    sent(dbuf, SUB, d_send)
    pltpu.make_async_copy(others, others, c_send).wait()
    for k in range(ns - 1):
        send_part(k).wait_send()


def per_device(nt, ns, fibre_points, shell_points, bending, shell_inverse):
    n_dev = nt * ns
    _, al, ql = shell_points.shape
    fib_groups = LANES // SUB
    nvec = ql // min(ql, LANES // al)
    vmem = pl.BlockSpec(memory_space=pltpu.VMEM)
    dma = pltpu.SemaphoreType.DMA
    block = shell_inverse.shape
    return pl.pallas_call(
        functools.partial(kernel, nt, ns),
        out_shape=(
            jax.ShapeDtypeStruct(fibre_points.shape, f32),
            jax.ShapeDtypeStruct(shell_points.shape, f32),
        ),
        in_specs=[vmem, vmem, vmem, pl.BlockSpec(memory_space=pltpu.HBM)],
        out_specs=(vmem, vmem),
        scratch_shapes=[
            pltpu.VMEM((ns, 3, al, ql) + block[3:], jnp.bfloat16),
            pltpu.VMEM((n_dev, SUB, LANES), f32),
            pltpu.VMEM((n_dev, SUB, LANES), f32),
            pltpu.VMEM((n_dev, SUB, LANES), f32),
            pltpu.VMEM((nt,) + block[3:], jnp.bfloat16),
            pltpu.VMEM((ns, 3, ql, LANES), f32),
            pltpu.VMEM((ns, 3, ql, LANES), f32),
            pltpu.VMEM((al, 3, ql, LANES), f32),
            pltpu.VMEM((fib_groups, 3, SUB, LANES), f32),
            pltpu.VMEM((n_dev, SUB, LANES), f32),
            pltpu.VMEM((n_dev, 6, SUB, LANES), f32),
            pltpu.VMEM((nt * nvec, 6, SUB, LANES), f32),
            pltpu.VMEM((fib_groups, 3, SUB, LANES), f32),
            pltpu.VMEM((LANES, LANES), f32),
            pltpu.VMEM((SUB, LANES), f32),
            pltpu.VMEM((SUB, LANES), f32),
            pltpu.VMEM(block[3:], jnp.bfloat16),
            pltpu.VMEM((SUB, LANES), f32),
            pltpu.VMEM((ql, LANES), jnp.int32),
            dma((ns,)), dma, dma((ns,)), dma, dma((ns,)), dma, dma, dma((ns,)), dma((ns,)),
            dma, dma((ns,)),
        ],
        compiler_params=pltpu.CompilerParams(
            collective_id=0, has_side_effects=True, vmem_limit_bytes=60 * 1024 * 1024
        ),
        name="shell_step",
    )(fibre_points, shell_points, bending, shell_inverse)


def solution(mesh):
    placed = (
        P(None, ("tgt", "src"), None),
        P(None, "tgt", "src"),
        P(),
        P(None, "tgt", None, None, "src", None),
    )
    return jax.shard_map(
        functools.partial(per_device, mesh.shape["tgt"], mesh.shape["src"]),
        mesh=mesh,
        in_specs=placed,
        out_specs=(P(None, ("tgt", "src"), None), P(None, "tgt", "src")),
        check_vma=False,
    )
```

```python
import functools
import math

import jax
import jax.numpy as jnp
from jax import lax
from jax.experimental import pallas as pl
from jax.experimental.pallas import tpu as pltpu
from jax.sharding import PartitionSpec as P

mobility = 1.0 / (8.0 * math.pi)
soften_sq = 0.0025
LANES = 128
SUB = 8
HIGHEST = lax.Precision.HIGHEST
MESH = pl.DeviceIdType.MESH
f32 = jnp.float32


def iotas(rows=SUB):
    lane = lax.broadcasted_iota(jnp.int32, (rows, LANES), 1)
    sub = lax.broadcasted_iota(jnp.int32, (rows, LANES), 0)
    return lane, sub


def flow(src_ref, start, count, targets, accs, unroll):
    unroll = math.gcd(unroll, count)

    def body(i, accs):
        accs = list(accs)
        for u in range(unroll):
            j = start + i * unroll + u
            sx, sy, sz, gx, gy, gz = [src_ref[j, c] for c in range(6)]
            for g, (tx, ty, tz) in enumerate(targets):
                dx, dy, dz = tx - sx, ty - sy, tz - sz
                q = dx * dx + dy * dy + (dz * dz + soften_sq)
                inv = lax.rsqrt(q)
                cubed = inv * inv * inv
                proj = (dx * gx + dy * gy + dz * gz) * cubed
                diag = (q + soften_sq) * cubed
                accs[3 * g] += diag * gx + proj * dx
                accs[3 * g + 1] += diag * gy + proj * dy
                accs[3 * g + 2] += diag * gz + proj * dz
        return tuple(accs)

    return lax.fori_loop(0, count // unroll, body, tuple(accs))


def fold_rows(rows, sub):
    def step(a, b, width):
        low = (sub & width) == 0
        up = a + pltpu.roll(a, SUB - width, 0)
        down = b + pltpu.roll(b, width, 0)
        return jnp.where(low, up, down)

    width = 4
    level = rows
    half = len(rows) // 2
    while half >= 1:
        level = [step(level[i], level[i + half], width) for i in range(half)]
        width //= 2
        half //= 2
    return level[0]


def kernel(
    nt, ns, fib_ref, shell_ref, bend_ref, mat_ref, vel_ref, den_ref,
    mat, gbuf, pbuf, dbuf, cbuf, part, rbuf, tbs, tbf, wide, src1, src2, fib_acc, weave,
    posblk, denblk, colblk, ptblk, lane_ref,
    mat_sem, g_send, g_recv, p_send, p_recv, c_send, c_recv, r_send, r_recv, d_send, d_recv,
):
    t, s = lax.axis_index("tgt"), lax.axis_index("src")
    n_dev = nt * ns
    al, ql = shell_ref.shape[1], shell_ref.shape[2]
    fl, nodes = fib_ref.shape[1], fib_ref.shape[2]
    fib_groups = LANES // SUB
    qv = min(ql, LANES // al)
    nvec = ql // qv
    lane_ref[...] = iotas(ql)[0]
    sub = iotas()[1]
    sub16 = iotas(ql)[1]
    lane, lane16 = lane_ref[pl.ds(0, SUB), :], lane_ref[...]

    def fetch(k):
        to = lax.rem(s + 1 + k, ns)
        return pltpu.make_async_copy(
            mat_ref.at[:, :, pl.ds(to * ql, ql)], mat.at[k], mat_sem.at[k]
        )

    for k in range(ns):
        fetch(k).start()

    def peer(i):
        return {"tgt": lax.rem(t + lax.rem(i, nt), nt), "src": lax.rem(s + i // nt, ns)}

    gbuf[...] = jnp.zeros_like(gbuf)
    barrier = pltpu.get_barrier_semaphore()

    def greet(i, _):
        pl.semaphore_signal(barrier, inc=1, device_id=peer(i), device_id_type=MESH)
        return 0

    lax.fori_loop(1, n_dev, greet, 0)

    ptblk[...] = jnp.zeros_like(ptblk)
    posblk[...] = jnp.zeros_like(posblk)
    denblk[...] = jnp.zeros_like(denblk)
    points = jnp.concatenate([fib_ref[:, f, :] for f in range(fl)], axis=1)
    ptblk[pl.ds(0, 3), :] = points
    bend = bend_ref[...]
    blank = jnp.zeros_like(bend)
    weave[...] = jnp.concatenate(
        [
            jnp.concatenate([bend if i == j else blank for j in range(fl)], axis=1)
            for i in range(fl)
        ],
        axis=0,
    )

    def spread(a, reps):
        out = []
        for c in range(3):
            row = shell_ref[c, pl.ds(a, 1), :]
            eye = lax.broadcasted_iota(jnp.int32, (ql, ql), 0) == lax.broadcasted_iota(
                jnp.int32, (ql, ql), 1
            )
            col = jnp.sum(jnp.where(eye, 1.0, 0.0) * row, axis=1, keepdims=True)
            wide_col = jnp.broadcast_to(col, (ql, LANES))
            tbs[a, c] = wide_col
            out.append(jnp.where(lax.rem(lane16, al) == a, wide_col, reps[c]))
        return tuple(out)

    reps = lax.fori_loop(0, al, spread, tuple(jnp.zeros((ql, LANES), f32) for _ in range(3)))

    def weave_rows(block, values):
        for c in range(3):
            for h in range(nvec):
                piece = values[c][h * qv:(h + 1) * qv]
                hit = lax.div(lane16[:qv], al) == sub16[:qv]
                block[pl.ds(c * nvec + h, 1), :] = jnp.sum(
                    jnp.where(hit, piece, 0.0), axis=0, keepdims=True
                )

    weave_rows(posblk, reps)

    def spread_fibre(g, _):
        for c in range(3):
            row = ptblk[pl.ds(c, 1), :]
            hit = jnp.where(lane == sub + g * SUB, 1.0, 0.0)
            col = jnp.sum(hit * row, axis=1, keepdims=True)
            tbf[g, c] = jnp.broadcast_to(col, (SUB, LANES))
        return 0

    lax.fori_loop(0, fib_groups, spread_fibre, 0)

    me = s * nt + t
    gbuf[me] = ptblk[...]
    pbuf[me] = posblk[...]
    pl.semaphore_wait(barrier, n_dev - 1)

    def spread_out(block, buf, rows, send, recv):
        def one(i, _):
            pltpu.make_async_remote_copy(
                src_ref=block.at[pl.ds(0, rows)],
                dst_ref=buf.at[me, pl.ds(0, rows)],
                send_sem=send,
                recv_sem=recv.at[s],
                device_id=peer(i),
                device_id_type=MESH,
            ).start()
            return 0

        lax.fori_loop(1, n_dev, one, 0)

    def arrived(buf, rows, recv, k):
        frm = lax.rem(s + k, ns)
        ref = buf.at[pl.ds(0, nt if k else nt - 1), pl.ds(0, rows)]
        pltpu.make_async_copy(ref, ref, recv.at[frm]).wait()

    def sent(buf, rows, send):
        ref = buf.at[pl.ds(0, n_dev - 1), pl.ds(0, rows)]
        pltpu.make_async_copy(ref, ref, send).wait()

    spread_out(ptblk, gbuf, 3, g_send, g_recv)
    spread_out(posblk, pbuf, SUB, p_send, p_recv)
    for k in range(ns):
        arrived(gbuf, 3, g_recv, k)

    all_points = gbuf[...].reshape(n_dev * SUB, LANES)
    wide[...] = (
        lax.dot_general(
            all_points, weave[...], (((1,), (1,)), ((), ())),
            precision=HIGHEST, preferred_element_type=f32,
        )
        * (-mobility)
    ).reshape(n_dev, SUB, LANES)

    def plane(j, _):
        for c in range(3):
            src1[j, c] = jnp.broadcast_to(gbuf[j, pl.ds(c, 1), :], (SUB, LANES))
            src1[j, c + 3] = jnp.broadcast_to(wide[j, pl.ds(c, 1), :], (SUB, LANES))
        return 0

    lax.fori_loop(0, n_dev, plane, 0)
    halves = ql // SUB
    zero = jnp.zeros((SUB, LANES), f32)

    def shell_targets(a, cols):
        groups = [
            tuple(tbs[a, c, pl.ds(h * SUB, SUB), :] for c in range(3)) for h in range(halves)
        ]
        accs = flow(src1, 0, n_dev, groups, [zero] * (3 * halves), 16)
        here = lane == t * al + a
        return tuple(
            jnp.where(here, jnp.sum(accs[i], axis=1, keepdims=True), cols[i])
            for i in range(3 * halves)
        )

    cols = lax.fori_loop(0, al, shell_targets, tuple([zero] * (3 * halves)))
    for c in range(3):
        colblk[c] = jnp.concatenate(
            [cols[3 * h + c] for h in range(halves)], axis=0
        ).astype(jnp.bfloat16)
    cbuf[t] = colblk[...]

    def send_cols(i, _):
        pltpu.make_async_remote_copy(
            src_ref=colblk, dst_ref=cbuf.at[t], send_sem=c_send, recv_sem=c_recv,
            device_id={"tgt": lax.rem(t + i, nt), "src": s}, device_id_type=MESH,
        ).start()
        return 0

    lax.fori_loop(1, nt, send_cols, 0)

    def fibre_targets(src_ref, start, count, first):
        def one(i, _):
            groups = [tuple(tbf[2 * i + h, c] for c in range(3)) for h in range(2)]
            accs = [
                zero if first else fib_acc[2 * i + h, c] for h in range(2) for c in range(3)
            ]
            accs = flow(src_ref, start, count, groups, accs, 16)
            for h in range(2):
                for c in range(3):
                    fib_acc[2 * i + h, c] = accs[3 * h + c]
            return 0

        lax.fori_loop(0, fib_groups // 2, one, 0)

    fibre_targets(src1, 0, n_dev, True)

    others = cbuf.at[pl.ds(0, nt - 1)]
    pltpu.make_async_copy(others, others, c_recv).wait()
    v = lax.fori_loop(
        0, nt, lambda i, total: total + cbuf[i].astype(f32), jnp.zeros(cbuf.shape[1:], f32)
    )

    def send_part(k):
        to = lax.rem(s + 1 + k, ns)
        return pltpu.make_async_remote_copy(
            src_ref=part.at[k], dst_ref=rbuf.at[k],
            send_sem=r_send.at[k], recv_sem=r_recv.at[k],
            device_id={"tgt": t, "src": to}, device_id_type=MESH,
        )

    def place(a, folded, dens):
        here = lax.rem(lane, al) == a
        return tuple(
            jnp.where(here, jnp.sum(y, axis=1, keepdims=True), d) for y, d in zip(folded, dens)
        )

    for k in range(ns):
        fetch(k).wait()

        def row_block(a, carry):
            folded, dens = carry
            dens = place(a - 1, folded, dens)
            new = []
            for x in range(3):
                for h in range(halves):
                    rows = []
                    for r in range(SUB):
                        prod = mat[k, x, a, h * SUB + r].astype(f32) * v
                        both = prod[0] + prod[1] + prod[2]
                        rows.append(
                            sum(both[i * SUB:(i + 1) * SUB] for i in range(halves))
                        )
                    new.append(fold_rows(rows, sub))
            return tuple(new), dens

        empty = tuple([zero] * (3 * halves))
        folded, dens = lax.fori_loop(0, al, row_block, (empty, empty))
        dens = place(al - 1, folded, dens)
        for x in range(3):
            for h in range(halves):
                part[k, x, pl.ds(h * SUB, SUB), :] = dens[x * halves + h]
        if k < ns - 1:
            send_part(k).start()

    total = part[ns - 1]
    for k in range(ns - 1):
        send_part(k).wait_recv()
        total = total + rbuf[k]
    total = -total
    weave_rows(denblk, [total[x] for x in range(3)])
    dbuf[me] = denblk[...]
    spread_out(denblk, dbuf, SUB, d_send, d_recv)

    pick = max(al, SUB)
    pl_lane, pl_sub = iotas(pick)
    eye = jnp.where(pl_lane == pl_sub, 1.0, 0.0).astype(f32)
    for x in range(3):
        den_ref[x] = lax.dot_general(
            eye, total[x], (((1,), (1,)), ((), ())), precision=HIGHEST, preferred_element_type=f32
        )[:al]

    for k in range(ns):
        arrived(pbuf, SUB, p_recv, k)
        arrived(dbuf, SUB, d_recv, k)
        base = lax.rem(s + k, ns) * nt

        def plane_back(j, _):
            for h in range(nvec):
                for c in range(3):
                    r = pl.ds(c * nvec + h, 1)
                    src2[j * nvec + h, c] = jnp.broadcast_to(pbuf[base + j, r, :], (SUB, LANES))
                    src2[j * nvec + h, c + 3] = jnp.broadcast_to(
                        dbuf[base + j, r, :] * mobility, (SUB, LANES)
                    )
            return 0

        lax.fori_loop(0, nt, plane_back, 0)
        fibre_targets(src2, 0, nt * nvec, False)

    def gather_rows(g, rows):
        hit = lane == sub + g * SUB
        return tuple(
            rows[c] + jnp.where(hit, jnp.sum(fib_acc[g, c], axis=1, keepdims=True), 0.0)
            for c in range(3)
        )

    rows = lax.fori_loop(0, fib_groups, gather_rows, (zero,) * 3)
    for c in range(3):
        row = jnp.sum(rows[c], axis=0, keepdims=True)
        for f in range(fl):
            vel_ref[c, pl.ds(f, 1), :] = row[:, f * nodes:(f + 1) * nodes]

    sent(gbuf, 3, g_send)
    sent(pbuf, SUB, p_send)
    sent(dbuf, SUB, d_send)
    pltpu.make_async_copy(others, others, c_send).wait()
    for k in range(ns - 1):
        send_part(k).wait_send()


def per_device(nt, ns, fibre_points, shell_points, bending, shell_inverse):
    n_dev = nt * ns
    _, al, ql = shell_points.shape
    fib_groups = LANES // SUB
    nvec = ql // min(ql, LANES // al)
    vmem = pl.BlockSpec(memory_space=pltpu.VMEM)
    dma = pltpu.SemaphoreType.DMA
    block = shell_inverse.shape
    return pl.pallas_call(
        functools.partial(kernel, nt, ns),
        out_shape=(
            jax.ShapeDtypeStruct(fibre_points.shape, f32),
            jax.ShapeDtypeStruct(shell_points.shape, f32),
        ),
        in_specs=[vmem, vmem, vmem, pl.BlockSpec(memory_space=pltpu.HBM)],
        out_specs=(vmem, vmem),
        scratch_shapes=[
            pltpu.VMEM((ns, 3, al, ql) + block[3:], jnp.bfloat16),
            pltpu.VMEM((n_dev, SUB, LANES), f32),
            pltpu.VMEM((n_dev, SUB, LANES), f32),
            pltpu.VMEM((n_dev, SUB, LANES), f32),
            pltpu.VMEM((nt,) + block[3:], jnp.bfloat16),
            pltpu.VMEM((ns, 3, ql, LANES), f32),
            pltpu.VMEM((ns, 3, ql, LANES), f32),
            pltpu.VMEM((al, 3, ql, LANES), f32),
            pltpu.VMEM((fib_groups, 3, SUB, LANES), f32),
            pltpu.VMEM((n_dev, SUB, LANES), f32),
            pltpu.VMEM((n_dev, 6, SUB, LANES), f32),
            pltpu.VMEM((nt * nvec, 6, SUB, LANES), f32),
            pltpu.VMEM((fib_groups, 3, SUB, LANES), f32),
            pltpu.VMEM((LANES, LANES), f32),
            pltpu.VMEM((SUB, LANES), f32),
            pltpu.VMEM((SUB, LANES), f32),
            pltpu.VMEM(block[3:], jnp.bfloat16),
            pltpu.VMEM((SUB, LANES), f32),
            pltpu.VMEM((ql, LANES), jnp.int32),
            dma((ns,)), dma, dma((ns,)), dma, dma((ns,)), dma, dma, dma((ns,)), dma((ns,)),
            dma, dma((ns,)),
        ],
        compiler_params=pltpu.CompilerParams(
            collective_id=0, has_side_effects=True, vmem_limit_bytes=60 * 1024 * 1024
        ),
        name="shell_step",
    )(fibre_points, shell_points, bending, shell_inverse)


def solution(mesh):
    placed = (
        P(None, ("tgt", "src"), None),
        P(None, "tgt", "src"),
        P(),
        P(None, "tgt", None, None, "src", None),
    )
    return jax.shard_map(
        functools.partial(per_device, mesh.shape["tgt"], mesh.shape["src"]),
        mesh=mesh,
        in_specs=placed,
        out_specs=(P(None, ("tgt", "src"), None), P(None, "tgt", "src")),
        check_vma=False,
    )
```
